32 devices in a mesh: fsdp: 16 (over z, x, core), tp: 2 (over y).
Axes of the slice: x: 2, y: 2, z: 4, core: 2. Of those that a mesh axis runs over, the one named last changes fastest.
Arguments:
- grad_iterate: bfloat16 [3584, 18432], P('tp', 'fsdp'), may hold values from -0.036828478 to 0.036828478
Outputs:
- update: float32 [3584, 18432], P('tp', 'fsdp')
The draws below stay inside these ranges and needn't reach their ends.
All inputs are finite; a program needn't handle non-finite values.
Results may differ from the reference program's by a relative error of at most 0.0031.
Values may be sent and summed in bfloat16 or wider, within the bound.
A program may use at most 128 MiB of HBM per device.

```python
import math
import jax
import jax.numpy as jnp

R = 3584
C = 18432


def draw_grad_iterate(key, part):
    key_one = jax.random.fold_in(key, 11)
    key_two = jax.random.fold_in(key, 23)
    key_four = jax.random.fold_in(key, 41)
    key_five = jax.random.fold_in(key, 53)
    key_six = jax.random.fold_in(key, 67)
    shared_rank = max(R // 4, 1)
    row_scale = jnp.exp(jax.random.uniform(key_two, (R, 1), jnp.float32, math.log(0.1), 0.0))
    factor_gain = jnp.exp(jax.random.uniform(key_six, (1, shared_rank), jnp.float32, math.log(0.4), math.log(1.6)))
    factor_gain = factor_gain / jnp.sqrt(jnp.mean(factor_gain * factor_gain))
    left_factor = jax.random.normal(key_four, (R, shared_rank), jnp.float32) * factor_gain
    right_factor = jax.random.normal(key_five, (shared_rank, C), jnp.float32)
    shared = jnp.dot(left_factor, right_factor) / math.sqrt(shared_rank)
    noise = jax.random.normal(key_one, (R, C), jnp.float32)
    entries = jnp.clip(0.25 * noise + 0.9 * shared, -3.5, 3.5)
    return (entries * row_scale / math.sqrt(C)).astype(jnp.bfloat16)


def setup_inputs(seed: int = 0) -> dict:
    arg_keys = jax.random.split(jax.random.key(seed), 2)
    return {
        "grad_iterate": draw_grad_iterate(jax.random.fold_in(arg_keys[1], 71), 0),
    }


quintic_one = 3.4445
quintic_three = -4.775
quintic_five = 2.0315

def reference(grad_iterate):
    gram = jnp.dot(grad_iterate, grad_iterate.T, preferred_element_type=jnp.float32)
    gram_low = gram.astype(jnp.bfloat16)
    applied = jnp.dot(gram_low, grad_iterate, preferred_element_type=jnp.float32)
    applied_low = applied.astype(jnp.bfloat16)
    twice_applied = jnp.dot(gram_low, applied_low, preferred_element_type=jnp.float32)
    mixed = quintic_one * grad_iterate.astype(jnp.float32) + quintic_three * applied + quintic_five * twice_applied
    return mixed * math.sqrt(C)
```

```python
import functools
import math

import jax
import jax.numpy as jnp
from jax import lax
from jax.experimental import pallas as pl
from jax.experimental.pallas import tpu as pltpu
from jax.sharding import PartitionSpec as P

quintic_one = 3.4445
quintic_three = -4.775
quintic_five = 2.0315

MESH = pl.DeviceIdType.MESH


def rows_by_rows(a, b):
    return lax.dot_general(a, b, (((1,), (1,)), ((), ())), preferred_element_type=jnp.float32)


def matmul(a, b):
    return jnp.dot(a, b, preferred_element_type=jnp.float32)


def general(grad_iterate, scale):
    columns = lax.all_gather(grad_iterate, "tp", axis=0, tiled=True)
    shares = lax.psum_scatter(
        rows_by_rows(columns, grad_iterate), "fsdp", scatter_dimension=0, tiled=True
    )
    gram_cols = lax.all_gather(shares.astype(jnp.bfloat16), "fsdp", axis=0, tiled=True)
    applied = lax.dot_general(
        gram_cols, columns, (((0,), (0,)), ((), ())), preferred_element_type=jnp.float32
    )
    twice_applied = matmul(
        gram_cols.T, lax.all_gather(applied.astype(jnp.bfloat16), "tp", axis=0, tiled=True)
    )
    mixed = (
        quintic_one * grad_iterate.astype(jnp.float32)
        + quintic_three * applied
        + quintic_five * twice_applied
    )
    return mixed * scale


def fused_kernel(
    nz, tile, scale,
    x_hbm, o_hbm,
    xg, xp, gram, out, cown, dxs, dxr, dzs, dzr, cxs, cxr, czs, czr,
    local_sem, ys, yr, cs, cr, dx_s, dx_r, dz_s, dz_r, cx_s, cx_r, cz_s, cz_r,
    daz_s, daz_r, dax_s, dax_r, dac_s, dac_r, day_s, day_r, dat_s, dat_r,
    cay_s, cay_r, caz_s, caz_r, cax_s, cax_r, cac_s, cac_r, out_sem,
):
    f = lax.axis_index("fsdp")
    y = lax.axis_index("tp")
    c = lax.rem(f, 2)
    xx = lax.rem(f // 2, 2)
    z = f // 4

    rows, width = xg.shape[1], xg.shape[2]
    half = rows // 2
    quarter = half // 2
    dpiece = half // nz
    cpiece = quarter // nz

    def device(z_, x_, c_, y_):
        return (z_ * 4 + x_ * 2 + c_, y_)

    to_y = device(z, xx, c, 1 - y)
    to_x = device(z, 1 - xx, c, y)
    to_c = device(z, xx, 1 - c, y)
    to_z = [device(lax.rem(z + k, nz), xx, c, y) for k in range(1, nz)]

    def remote(src, dst, ssem, rsem, target):
        return pltpu.make_async_remote_copy(
            src_ref=src, dst_ref=dst, send_sem=ssem, recv_sem=rsem,
            device_id=target, device_id_type=MESH,
        )

    load = pltpu.make_async_copy(x_hbm, xg.at[y], local_sem)
    load.start()
    barrier = pltpu.get_barrier_semaphore()
    peers = [to_y, to_x, to_c] + to_z
    for peer in peers:
        pl.semaphore_signal(barrier, inc=1, device_id=peer, device_id_type=MESH)
    pl.semaphore_wait(barrier, len(peers))
    load.wait()

    sends = []

    def begin(copy):
        copy.start()
        sends.append(copy)
        return copy

    def al(i, m):
        return pl.multiple_of(i, m)

    share = begin(remote(xg.at[y], xp.at[y], cs.at[0], cr.at[0], to_c))
    over = []
    for s in range(2):
        h = (1 - y) if s == 0 else y
        block = xg.at[y, pl.ds(al(h * half, half), half)]
        over.append(begin(remote(block, block, ys.at[s], yr.at[s], to_y)))
    share.wait_recv()

    cols = pl.ds(al(c * half, half), half)

    def gram_part(left, lrow, n, right, rrow):
        l = pl.ds(lrow, n)
        r = pl.ds(rrow, half)
        return rows_by_rows(xg[left, l, :], xg[right, r, :]) + rows_by_rows(
            xp[left, l, :], xp[right, r, :]
        )

    def order(p):
        return lax.rem(z + 1 + p, nz)

    chalf = al(c * half, half)

    def d_copy(p):
        t = order(p)
        return remote(dxs.at[t], dxr.at[t], dx_s.at[p], dx_r.at[p], to_x)

    def d_send(p, _):
        t = order(p)
        dxs[t] = gram_part(y, al((1 - xx) * half + t * dpiece, dpiece), dpiece, y, chalf).astype(
            jnp.bfloat16
        )
        d_copy(p).start()
        return 0

    lax.fori_loop(0, nz, d_send, 0)

    def d_own(p, _):
        t = order(p)
        out[pl.ds(al(t * dpiece, dpiece), dpiece), 0:half] = gram_part(
            y, al(xx * half + t * dpiece, dpiece), dpiece, y, chalf
        )
        return 0

    lax.fori_loop(0, nz, d_own, 0)

    dz = []
    for p in range(nz):
        t = order(p)
        d_copy(p).wait()
        place = pl.ds(al(t * dpiece, dpiece), dpiece)
        total = out[place, 0:half] + dxr[t].astype(jnp.float32)
        if p < nz - 1:
            dzs[p] = total.astype(jnp.bfloat16)
            dz.append(begin(remote(dzs.at[p], dzr.at[p], dz_s.at[p], dz_r.at[p], to_z[p])))
        else:
            out[place, 0:half] = total
    total = out[pl.ds(al(z * dpiece, dpiece), dpiece), 0:half]
    for p in range(nz - 1):
        dz[p].wait_recv()
        total = total + dzr[p].astype(jnp.float32)

    def d_slab(who, x_, z_):
        return gram.at[3 * who, pl.ds(al(x_ * half + z_ * dpiece, dpiece), dpiece), cols]

    gram[3 * y, pl.ds(al(xx * half + z * dpiece, dpiece), dpiece), cols] = total.astype(
        jnp.bfloat16
    )

    mine = d_slab(y, xx, z)
    daz = [
        begin(remote(mine, mine, daz_s.at[k], daz_r.at[k], to_z[k])) for k in range(nz - 1)
    ]
    dax, dac, day = [], [], []
    for k in range(nz):
        if k > 0:
            daz[k - 1].wait_recv()
        here = d_slab(y, xx, lax.rem(z - k + nz, nz))
        dax.append(begin(remote(here, here, dax_s.at[k], dax_r.at[k], to_x)))
        dac.append(begin(remote(here, here, dac_s.at[k], dac_r.at[k], to_c)))
        day.append(begin(remote(here, here, day_s.at[k], day_r.at[k], to_y)))

    for s in range(2):
        over[s].wait_recv()
    fwd = (1 - y) * (1 - c) + y
    block = pl.ds(al(fwd * half, half), half)
    cfwd = begin(remote(xg.at[1 - y, block], xp.at[1 - y, block], cs.at[1], cr.at[1], to_c))
    cfwd.wait_recv()

    def c_copy(p):
        t = order(p)
        return remote(cxs.at[t], cxr.at[t], cx_s.at[p], cx_r.at[p], to_x)

    def c_send(p, _):
        t = order(p)
        cxs[t] = gram_part(
            0, al(y * half + (1 - xx) * quarter + t * cpiece, cpiece), cpiece, 1, chalf
        ).astype(jnp.bfloat16)
        c_copy(p).start()
        return 0

    lax.fori_loop(0, nz, c_send, 0)

    def c_own(p, _):
        t = order(p)
        cown[t] = gram_part(
            0, al(y * half + xx * quarter + t * cpiece, cpiece), cpiece, 1, chalf
        )
        return 0

    lax.fori_loop(0, nz, c_own, 0)

    cz = []
    for p in range(nz):
        t = order(p)
        c_copy(p).wait()
        total = cown[t] + cxr[t].astype(jnp.float32)
        if p < nz - 1:
            czs[p] = total.astype(jnp.bfloat16)
            cz.append(begin(remote(czs.at[p], czr.at[p], cz_s.at[p], cz_r.at[p], to_z[p])))
        else:
            cown[t] = total

    for k in range(nz):
        dax[k].wait_recv()
        here = d_slab(y, 1 - xx, lax.rem(z - k + nz, nz))
        dac.append(begin(remote(here, here, dac_s.at[nz + k], dac_r.at[nz + k], to_c)))

    total = cown[z]
    for p in range(nz - 1):
        cz[p].wait_recv()
        total = total + czr[p].astype(jnp.float32)

    def c_slab(who, x_, z_):
        return gram.at[
            1, pl.ds(al(who * half + x_ * quarter + z_ * cpiece, cpiece), cpiece), cols
        ]

    gram[1, pl.ds(al(y * half + xx * quarter + z * cpiece, cpiece), cpiece), cols] = total.astype(
        jnp.bfloat16
    )
    mine = c_slab(y, xx, z)
    cay = begin(remote(mine, mine, cay_s, cay_r, to_y))
    caz, cax, cac = [], [], []
    for k in range(nz - 1):
        caz.append(begin(remote(mine, mine, caz_s.at[k], caz_r.at[k], to_z[k])))
    cax.append(begin(remote(mine, mine, cax_s.at[0], cax_r.at[0], to_x)))
    cac.append(begin(remote(mine, mine, cac_s.at[0], cac_r.at[0], to_c)))
    cay.wait_recv()
    theirs = c_slab(1 - y, xx, z)
    for k in range(nz - 1):
        j = nz - 1 + k
        caz.append(begin(remote(theirs, theirs, caz_s.at[j], caz_r.at[j], to_z[k])))
    cax.append(begin(remote(theirs, theirs, cax_s.at[1], cax_r.at[1], to_x)))
    cac.append(begin(remote(theirs, theirs, cac_s.at[1], cac_r.at[1], to_c)))
    for k in range(nz):
        here = d_slab(y, 1 - xx, lax.rem(z - k + nz, nz))
        day.append(begin(remote(here, here, day_s.at[nz + k], day_r.at[nz + k], to_y)))

    for copy in dac:
        copy.wait_recv()

    def tile_of(i):
        return pl.ds(al(i * tile, tile), tile)

    def first(i, _):
        m = tile_of(i)
        out[m, :] = matmul(gram[3 * y, m, :], xg[y])
        return 0

    lax.fori_loop(0, rows // tile, first, 0)

    n = 2
    for k in range(1, nz):
        for w in range(2):
            caz[w * (nz - 1) + k - 1].wait_recv()
            who = y if w == 0 else 1 - y
            here = c_slab(who, xx, lax.rem(z - k + nz, nz))
            cax.append(begin(remote(here, here, cax_s.at[n], cax_r.at[n], to_x)))
            cac.append(begin(remote(here, here, cac_s.at[n], cac_r.at[n], to_c)))
            n += 1
    dat = []
    for k in range(nz):
        day[k].wait_recv()
        here = d_slab(1 - y, xx, lax.rem(z - k + nz, nz))
        dat.append(begin(remote(here, here, dat_s.at[k], dat_r.at[k], to_c)))
    for j in range(2 * nz):
        cax[j].wait_recv()
        k, w = j // 2, j % 2
        who = y if w == 0 else 1 - y
        here = c_slab(who, 1 - xx, lax.rem(z - k + nz, nz))
        cac.append(begin(remote(here, here, cac_s.at[n], cac_r.at[n], to_c)))
        n += 1
    for copy in cac:
        copy.wait_recv()

    def flip(i, _):
        m = tile_of(i)
        gram[2, m, :] = gram[1, :, m].T
        return 0

    lax.fori_loop(0, rows // tile, flip, 0)

    def second(i, _):
        m = tile_of(i)
        total = out[m, :] + matmul(gram[2 * y + 1 - y, m, :], xg[1 - y])
        xp[y, m, :] = total.astype(jnp.bfloat16)
        out[m, :] = (
            quintic_one * xg[y, m, :].astype(jnp.float32) + quintic_three * total
        )
        return 0

    lax.fori_loop(0, rows // tile, second, 0)

    for k in range(nz):
        day[nz + k].wait_recv()
        here = d_slab(1 - y, 1 - xx, lax.rem(z - k + nz, nz))
        dat.append(begin(remote(here, here, dat_s.at[nz + k], dat_r.at[nz + k], to_c)))
    for copy in dat:
        copy.wait_recv()

    def third(i, _):
        m = tile_of(i)
        xp[1 - y, m, :] = (
            matmul(gram[2 * (1 - y) + y, m, :], xg[y])
            + matmul(gram[3 * (1 - y), m, :], xg[1 - y])
        ).astype(jnp.bfloat16)
        return 0

    lax.fori_loop(0, rows // tile, third, 0)

    def back(i):
        m = tile_of(i)
        return pltpu.make_async_copy(out.at[m], o_hbm.at[m], out_sem.at[i])

    def fourth(i, _):
        m = tile_of(i)
        twice = matmul(gram[2 * y, m, :], xp[0]) + matmul(gram[2 * y + 1, m, :], xp[1])
        out[m, :] = (out[m, :] + quintic_five * twice) * scale
        back(i).start()
        return 0

    lax.fori_loop(0, rows // tile, fourth, 0)

    for copy in sends:
        copy.wait_send()

    def finish(i, _):
        back(i).wait()
        return 0

    lax.fori_loop(0, rows // tile, finish, 0)


def fused(mesh, grad_iterate, scale):
    rows, width = grad_iterate.shape
    nz = mesh.shape["fsdp"] // 4
    half, quarter = rows // 2, rows // 4
    dpiece, cpiece = half // nz, quarter // nz
    tile = next(t for t in (256, 128) if rows % t == 0)
    bf16, f32 = jnp.bfloat16, jnp.float32
    dma = pltpu.SemaphoreType.DMA
    scratch = [
        pltpu.VMEM((2, rows, width), bf16),
        pltpu.VMEM((2, rows, width), bf16),
        pltpu.VMEM((4, rows, rows), bf16),
        pltpu.VMEM((rows, width), f32),
        pltpu.VMEM((nz, cpiece, half), f32),
        pltpu.VMEM((nz, dpiece, half), bf16),
        pltpu.VMEM((nz, dpiece, half), bf16),
        pltpu.VMEM((nz - 1, dpiece, half), bf16),
        pltpu.VMEM((nz - 1, dpiece, half), bf16),
        pltpu.VMEM((nz, cpiece, half), bf16),
        pltpu.VMEM((nz, cpiece, half), bf16),
        pltpu.VMEM((nz - 1, cpiece, half), bf16),
        pltpu.VMEM((nz - 1, cpiece, half), bf16),
        dma,
    ]
    pairs = [2, 2, nz, nz - 1, nz, nz - 1, nz - 1, nz, 2 * nz, 2 * nz, 2 * nz,
             None, 2 * (nz - 1), 2 * nz, 4 * nz]
    for count in pairs:
        scratch += [dma if count is None else dma((count,))] * 2
    scratch.append(dma((rows // tile,)))
    flops = 2 * rows * rows * width * 7
    return pl.pallas_call(
        functools.partial(fused_kernel, nz, tile, scale),
        out_shape=jax.ShapeDtypeStruct((rows, width), f32),
        in_specs=[pl.BlockSpec(memory_space=pl.ANY)],
        out_specs=pl.BlockSpec(memory_space=pl.ANY),
        scratch_shapes=scratch,
        compiler_params=pltpu.CompilerParams(
            collective_id=0, has_side_effects=True, vmem_limit_bytes=67043328
        ),
        cost_estimate=pl.CostEstimate(
            flops=flops, bytes_accessed=6 * rows * width, transcendentals=0
        ),
    )(grad_iterate)


def fits(mesh, shape):
    rows, width = shape
    devices = mesh.shape["fsdp"]
    if mesh.shape["tp"] != 2 or devices % 4 or devices < 8:
        return False
    nz = devices // 4
    if rows % 256 or rows // 2 > width or width % 128 or (rows // 4) % (16 * nz):
        return False
    return 12 * rows * width + 8 * rows * rows + 4 * rows * rows < 64 * 2**20


def solution(mesh):
    def local(scale, grad_iterate):
        if fits(mesh, grad_iterate.shape):
            return fused(mesh, grad_iterate, scale)
        return general(grad_iterate, scale)

    def whole(grad_iterate):
        scale = math.sqrt(grad_iterate.shape[1])
        return jax.shard_map(
            functools.partial(local, scale),
            mesh=mesh,
            in_specs=(P("tp", "fsdp"),),
            out_specs=P("tp", "fsdp"),
            check_vma=False,
        )(grad_iterate)

    return whole
```

```python
import functools
import math

import jax
import jax.numpy as jnp
from jax import lax
from jax.experimental import pallas as pl
from jax.experimental.pallas import tpu as pltpu
from jax.sharding import PartitionSpec as P

quintic_one = 3.4445
quintic_three = -4.775
quintic_five = 2.0315

MESH = pl.DeviceIdType.MESH


def rows_by_rows(a, b):
    return lax.dot_general(a, b, (((1,), (1,)), ((), ())), preferred_element_type=jnp.float32)


def columns_by_rows(a, b):
    return lax.dot_general(a, b, (((0,), (0,)), ((), ())), preferred_element_type=jnp.float32)


def matmul(a, b):
    return jnp.dot(a, b, preferred_element_type=jnp.float32)


def general(grad_iterate, scale):
    columns = lax.all_gather(grad_iterate, "tp", axis=0, tiled=True)
    shares = lax.psum_scatter(
        rows_by_rows(columns, grad_iterate), "fsdp", scatter_dimension=0, tiled=True
    )
    gram_cols = lax.all_gather(shares.astype(jnp.bfloat16), "fsdp", axis=0, tiled=True)
    applied = lax.dot_general(
        gram_cols, columns, (((0,), (0,)), ((), ())), preferred_element_type=jnp.float32
    )
    twice_applied = matmul(
        gram_cols.T, lax.all_gather(applied.astype(jnp.bfloat16), "tp", axis=0, tiled=True)
    )
    mixed = (
        quintic_one * grad_iterate.astype(jnp.float32)
        + quintic_three * applied
        + quintic_five * twice_applied
    )
    return mixed * scale


def fused_kernel(
    nz, tile, scale,
    x_hbm, o_hbm,
    xg, xp, gram, acc, dxs, dxr, dzs, dzr, cxs, cxr, czs, czr,
    local_sem, ys, yr, cs, cr, dx_s, dx_r, dz_s, dz_r, cx_s, cx_r, cz_s, cz_r,
    dey_s, dey_r, daz_s, daz_r, dtz_s, dtz_r, dax_s, dax_r, dtx_s, dtx_r,
    dac_s, dac_r, dtc_s, dtc_r, dly_s, dly_r, dlc_s, dlc_r,
    cay_s, cay_r, caz_s, caz_r, cax_s, cax_r, cac_s, cac_r, out_sem,
):
    f = lax.axis_index("fsdp")
    y = lax.axis_index("tp")
    c = lax.rem(f, 2)
    xx = lax.rem(f // 2, 2)
    z = f // 4

    rows = xg.shape[1]
    half = rows // 2
    quarter = half // 2
    dpiece = half // nz
    cpiece = quarter // nz

    def device(z_, x_, c_, y_):
        return (z_ * 4 + x_ * 2 + c_, y_)

    to_y = device(z, xx, c, 1 - y)
    to_x = device(z, 1 - xx, c, y)
    to_c = device(z, xx, 1 - c, y)
    to_z = [device(lax.rem(z + k, nz), xx, c, y) for k in range(1, nz)]

    def remote(src, dst, ssem, rsem, target):
        return pltpu.make_async_remote_copy(
            src_ref=src, dst_ref=dst, send_sem=ssem, recv_sem=rsem,
            device_id=target, device_id_type=MESH,
        )

    load = pltpu.make_async_copy(x_hbm, xg.at[y], local_sem)
    load.start()
    barrier = pltpu.get_barrier_semaphore()
    peers = [to_y, to_x, to_c] + to_z
    for peer in peers:
        pl.semaphore_signal(barrier, inc=1, device_id=peer, device_id_type=MESH)
    pl.semaphore_wait(barrier, len(peers))
    load.wait()

    sends = []

    def begin(copy):
        copy.start()
        sends.append(copy)
        return copy

    def move(block, ssem, rsem, target):
        return begin(remote(block, block, ssem, rsem, target))

    def at(i, n):
        return pl.ds(pl.multiple_of(i, n if n < 128 else 16), n)

    def back_from(k):
        return lax.rem(z - k + nz, nz)

    share = begin(remote(xg.at[y], xp.at[y], cs.at[0], cr.at[0], to_c))

    def x_block(s):
        h = (1 - y) if s < 2 else y
        return xg.at[y, at(h * half + (s % 2) * quarter, quarter)]

    over = [move(x_block(s), ys.at[s], yr.at[s], to_y) for s in range(3)]
    share.wait_recv()

    cols = pl.ds(pl.multiple_of(c * half, 128), half)
    rhs = at(c * half, half)

    def gram_part(left, lrow, n, right):
        l = at(lrow, n)
        return rows_by_rows(xg[left, l, :], xg[right, rhs, :]) + rows_by_rows(
            xp[left, l, :], xp[right, rhs, :]
        )

    def order(p):
        return lax.rem(z + 1 + p, nz)

    def d_copy(p):
        t = order(p)
        return remote(dxs.at[t], dxr.at[t], dx_s.at[p], dx_r.at[p], to_x)

    def d_send(p, _):
        t = order(p)
        dxs[t] = gram_part(y, (1 - xx) * half + t * dpiece, dpiece, y).astype(jnp.bfloat16)
        d_copy(p).start()
        return 0

    lax.fori_loop(0, nz, d_send, 0)

    def d_own(p, _):
        t = order(p)
        acc[y, at(t * dpiece, dpiece), 0:half] = gram_part(
            y, xx * half + t * dpiece, dpiece, y
        )
        return 0

    lax.fori_loop(0, nz, d_own, 0)

    dz = []
    for p in range(nz):
        t = order(p)
        d_copy(p).wait()
        place = at(t * dpiece, dpiece)
        total = acc[y, place, 0:half] + dxr[t].astype(jnp.float32)
        if p < nz - 1:
            dzs[p] = total.astype(jnp.bfloat16)
            dz.append(begin(remote(dzs.at[p], dzr.at[p], dz_s.at[p], dz_r.at[p], to_z[p])))
        else:
            acc[y, place, 0:half] = total

    for s in range(2):
        over[s].wait_recv()
    fwd = (1 - y) * (1 - c) + y
    block = at(fwd * half, half)
    cfwd = remote(xg.at[1 - y, block], xp.at[1 - y, block], cs.at[1], cr.at[1], to_c)
    sends.append(cfwd)
    late_send = jnp.logical_and(y == 0, c == 0)
    late_c = jnp.logical_and(y == 0, c == 1)

    @pl.when(jnp.logical_not(late_send))
    def _():
        cfwd.start()

    def c_copy(t):
        return remote(cxs.at[t], cxr.at[t], cx_s.at[t], cx_r.at[t], to_x)

    def cz_copy(p):
        return remote(czs.at[p], czr.at[p], cz_s.at[p], cz_r.at[p], to_z[p])

    def c_compute():
        cfwd.wait_recv()
        part = gram_part(0, y * half + (1 - xx) * quarter, quarter, 1)
        for t in range(nz):
            cxs[t] = part[t * cpiece:(t + 1) * cpiece].astype(jnp.bfloat16)
        for t in range(nz):
            c_copy(t).start()
        acc[1 - y, 0:quarter, 0:half] = gram_part(0, y * half + xx * quarter, quarter, 1)

    def c_exchange():
        for t in range(nz):
            c_copy(t).wait()
        for p in range(nz - 1):
            t = order(p)
            czs[p] = (
                acc[1 - y, at(t * cpiece, cpiece), 0:half] + cxr[t].astype(jnp.float32)
            ).astype(jnp.bfloat16)
            cz_copy(p).start()

    def c_slab(who, x_, z_):
        return (1, at(who * half + x_ * quarter + z_ * cpiece, cpiece), cols)

    cmine = gram.at[c_slab(y, xx, z)]
    cay = remote(cmine, cmine, cay_s, cay_r, to_y)

    def c_finish():
        total = acc[1 - y, at(z * cpiece, cpiece), 0:half] + cxr[z].astype(jnp.float32)
        for p in range(nz - 1):
            cz_copy(p).wait()
            total = total + czr[p].astype(jnp.float32)
        gram[c_slab(y, xx, z)] = total.astype(jnp.bfloat16)
        cay.start()

    @pl.when(jnp.logical_not(late_c))
    def _():
        c_compute()

    def d_slab(who, x_, z_):
        return (2 * who, at(x_ * half + z_ * dpiece, dpiece), cols)

    def d_part(who, x_, z_, part):
        return (2 * who, at(x_ * half + z_ * dpiece + part * cpiece, cpiece), cols)

    total = acc[y, at(z * dpiece, dpiece), 0:half]
    for p in range(nz - 1):
        dz[p].wait_recv()
        total = total + dzr[p].astype(jnp.float32)
    gram[d_slab(y, xx, z)] = total.astype(jnp.bfloat16)

    dey = move(gram.at[d_part(y, xx, z, 0)], dey_s, dey_r, to_y)
    over.append(move(x_block(3), ys.at[3], yr.at[3], to_y))
    daz, dax, dac, dtz, dtx, dtc, dly, dlc = [], [], [], [], [], [], [], []

    def pass_own(k):
        here = gram.at[d_slab(y, xx, back_from(k))]
        dax.append(move(here, dax_s.at[k], dax_r.at[k], to_x))
        dac.append(move(here, dac_s.at[k], dac_r.at[k], to_c))

    def pass_theirs(k):
        here = gram.at[d_part(1 - y, xx, back_from(k), 0)]
        dtx.append(move(here, dtx_s.at[k], dtx_r.at[k], to_x))
        dtc.append(move(here, dtc_s.at[k], dtc_r.at[k], to_c))

    def pass_late(k, x_):
        here = gram.at[d_part(y, x_, back_from(k % nz), 1)]
        dly.append(move(here, dly_s.at[k], dly_r.at[k], to_y))

    dmine = gram.at[d_slab(y, xx, z)]

    def spread_own(k):
        daz.append(move(dmine, daz_s.at[k], daz_r.at[k], to_z[k]))

    pass_own(0)
    spread_own(0)

    @pl.when(jnp.logical_not(late_c))
    def _():
        c_exchange()

    for k in range(1, nz - 1):
        spread_own(k)
    dey.wait_recv()
    dtheirs = gram.at[d_part(1 - y, xx, z, 0)]
    for k in range(nz - 1):
        dtz.append(move(dtheirs, dtz_s.at[k], dtz_r.at[k], to_z[k]))
    daz[0].wait_recv()
    pass_own(1)
    pass_theirs(0)

    @pl.when(jnp.logical_not(late_c))
    def _():
        c_finish()

    pass_late(0, xx)
    pass_late(1, xx)
    def c_move(who, k, target, ssem, rsem):
        here = gram.at[c_slab(who, xx, back_from(k))]
        return remote(here, here, ssem, rsem, target)

    def c_over_z(who, k):
        j = who * (nz - 1) + k
        return c_move(who, 0, to_z[k], caz_s.at[j], caz_r.at[j])

    def c_over_x(who, k):
        j = who * nz + k
        return c_move(who, k, to_x, cax_s.at[j], cax_r.at[j])

    def c_over_c(who, k):
        j = who * nz + k
        return c_move(who, k, to_c, cac_s.at[j], cac_r.at[j])

    def c_spread(who):
        @pl.when(y == 1 - who)
        def _():
            cay.wait_recv()

        for k in range(nz - 1):
            c_over_z(who, k).start()
        c_over_x(who, 0).start()
        c_over_c(who, 0).start()

    for s in range(2, 4):
        over[s].wait_recv()

    @pl.when(late_send)
    def _():
        cfwd.start()

    @pl.when(late_c)
    def _():
        c_compute()

    c_spread(1)

    @pl.when(c == 0)
    def _():
        c_spread(0)

    for k in range(2, nz):
        daz[k - 1].wait_recv()
        pass_own(k)
        pass_late(k, xx)

    @pl.when(late_c)
    def _():
        c_exchange()

    dtz[0].wait_recv()
    pass_theirs(1)

    def d_from_x(k):
        dax[k].wait_recv()
        here = gram.at[d_slab(y, 1 - xx, back_from(k))]
        dac.append(move(here, dac_s.at[nz + k], dac_r.at[nz + k], to_c))
        pass_late(nz + k, 1 - xx)

    d_from_x(0)
    for k in range(2, nz):
        dtz[k - 1].wait_recv()
        pass_theirs(k)
        d_from_x(k - 1)

    @pl.when(late_c)
    def _():
        c_finish()

    d_from_x(nz - 1)

    @pl.when(c == 1)
    def _():
        c_spread(0)

    for k in range(nz):
        dtx[k].wait_recv()
        here = gram.at[d_part(1 - y, 1 - xx, back_from(k), 0)]
        dtc.append(move(here, dtc_s.at[nz + k], dtc_r.at[nz + k], to_c))
    for copy in dac:
        copy.wait_recv()

    def tile_of(i):
        return at(i * tile, tile)

    tiles = rows // tile

    def diagonal(side, first, count):
        def body(i, _):
            m = tile_of(i)
            acc[side, m, :] = matmul(gram[2 * side, m, :], xg[side])
            return 0

        lax.fori_loop(first, first + count, body, 0)

    def share_out(side, events):
        done = 0
        for n, event in enumerate(events):
            upto = tiles * (n + 1) // len(events)
            if upto > done:
                diagonal(side, done, upto - done)
            done = upto
            event()

    def c_pass(who, k):
        def event():
            c_over_z(who, k - 1).wait_recv()
            c_over_x(who, k).start()
            c_over_c(who, k).start()

        return event

    def d_late(k):
        def event():
            dly[k].wait_recv()
            here = gram.at[d_part(1 - y, xx if k < nz else 1 - xx, back_from(k % nz), 1)]
            dlc.append(move(here, dlc_s.at[k], dlc_r.at[k], to_c))

        return event

    def c_from_x(who, k):
        def event():
            c_over_x(who, k).wait_recv()
            j = (2 + who) * nz + k
            here = gram.at[c_slab(who, 1 - xx, back_from(k))]
            far[who].append(move(here, cac_s.at[j], cac_r.at[j], to_c))

        return event

    def cross(x_, who, last):
        m = at(who * half + x_ * quarter, quarter)
        total = acc[0, m, :] + matmul(gram[1, m, :], xg[1])
        acc[0, m, :] = total
        xp[0, m, :] = total.astype(jnp.bfloat16)

        def body(i, _):
            n = tile_of(i)
            ncol = pl.ds(pl.multiple_of(i * tile, 128), tile)
            total = acc[1, n, :] + columns_by_rows(gram[1, m, ncol], xg[0, m, :])
            acc[1, n, :] = total
            if last:
                xp[1, n, :] = total.astype(jnp.bfloat16)
            return 0

        lax.fori_loop(0, tiles, body, 0)

    def cross_own(who):
        for k in range(nz):
            c_over_c(who, k).wait_recv()
        cross(xx, who, False)

    def cross_far(who, last):
        for copy in far[who]:
            copy.wait_recv()
        cross(1 - xx, who, last)

    far = [[], []]
    share_out(y, [c_pass(1, k) for k in range(1, nz)])
    for k in range(2 * nz):
        d_late(k)()
    for copy in dtc + dlc:
        copy.wait_recv()
    share_out(
        1 - y,
        [c_from_x(1, k) for k in range(nz)] + [c_pass(0, k) for k in range(1, nz)],
    )
    cross_own(1)
    cross_far(1, False)
    for k in range(nz):
        c_from_x(0, k)()
    cross_own(0)
    cross_far(0, True)

    def back(i):
        m = tile_of(i)
        return pltpu.make_async_copy(acc.at[y, m], o_hbm.at[m], out_sem.at[i])

    def finish(m, twice):
        acc[y, m, :] = (
            quintic_one * xg[y, m, :].astype(jnp.float32)
            + quintic_three * acc[y, m, :]
            + quintic_five * twice
        ) * scale

    @pl.when(y == 0)
    def _():
        def body(i, _):
            m = tile_of(i)
            finish(m, matmul(gram[0, m, :], xp[0]) + matmul(gram[1, m, :], xp[1]))
            back(i).start()
            return 0

        lax.fori_loop(0, rows // tile, body, 0)

    @pl.when(y == 1)
    def _():
        def body(i, _):
            m = tile_of(i)
            ncol = pl.ds(pl.multiple_of(i * tile, 128), tile)
            finish(m, columns_by_rows(gram[1, :, ncol], xp[0]) + matmul(gram[2, m, :], xp[1]))
            back(i).start()
            return 0

        lax.fori_loop(0, rows // tile, body, 0)

    for who in range(2):
        for k in range(nz - 1):
            sends.append(c_over_z(who, k))
        for k in range(nz):
            sends += [c_over_x(who, k), c_over_c(who, k)]
    for copy in sends + [cay]:
        copy.wait_send()

    def drain(i, _):
        back(i).wait()
        return 0

    lax.fori_loop(0, rows // tile, drain, 0)


def fused(mesh, grad_iterate, scale):
    rows, width = grad_iterate.shape
    nz = mesh.shape["fsdp"] // 4
    half, quarter = rows // 2, rows // 4
    dpiece, cpiece = half // nz, quarter // nz
    tile = next(t for t in (256, 128) if rows % t == 0)
    bf16, f32 = jnp.bfloat16, jnp.float32
    dma = pltpu.SemaphoreType.DMA
    scratch = [
        pltpu.VMEM((2, rows, width), bf16),
        pltpu.VMEM((2, rows, width), bf16),
        pltpu.VMEM((3, rows, rows), bf16),
        pltpu.VMEM((2, rows, width), f32),
        pltpu.VMEM((nz, dpiece, half), bf16),
        pltpu.VMEM((nz, dpiece, half), bf16),
        pltpu.VMEM((nz - 1, dpiece, half), bf16),
        pltpu.VMEM((nz - 1, dpiece, half), bf16),
        pltpu.VMEM((nz, cpiece, half), bf16),
        pltpu.VMEM((nz, cpiece, half), bf16),
        pltpu.VMEM((nz - 1, cpiece, half), bf16),
        pltpu.VMEM((nz - 1, cpiece, half), bf16),
        dma,
    ]
    counts = dict(
        y=4, c=2, dx=nz, dz=nz - 1, cx=nz, cz=nz - 1, dey=None, daz=nz - 1, dtz=nz - 1,
        dax=nz, dtx=nz, dac=2 * nz, dtc=2 * nz, dly=2 * nz, dlc=2 * nz,
        cay=None, caz=2 * (nz - 1), cax=2 * nz, cac=4 * nz,
    )
    for count in counts.values():
        scratch += [dma if count is None else dma((count,))] * 2
    scratch.append(dma((rows // tile,)))
    flops = 2 * rows * rows * width * 7
    return pl.pallas_call(
        functools.partial(fused_kernel, nz, tile, scale),
        out_shape=jax.ShapeDtypeStruct((rows, width), f32),
        in_specs=[pl.BlockSpec(memory_space=pl.ANY)],
        out_specs=pl.BlockSpec(memory_space=pl.ANY),
        scratch_shapes=scratch,
        compiler_params=pltpu.CompilerParams(
            collective_id=0, has_side_effects=True, vmem_limit_bytes=67043328
        ),
        cost_estimate=pl.CostEstimate(
            flops=flops, bytes_accessed=6 * rows * width, transcendentals=0
        ),
    )(grad_iterate)


def fits(mesh, shape):
    rows, width = shape
    devices = mesh.shape["fsdp"]
    if mesh.shape["tp"] != 2 or devices % 4 or devices < 8:
        return False
    nz = devices // 4
    if rows % 256 or rows // 2 > width or width % 128 or (rows // 4) % (16 * nz):
        return False
    return 16 * rows * width + 8 * rows * rows < 60 * 2**20


def solution(mesh):
    def local(scale, grad_iterate):
        if fits(mesh, grad_iterate.shape):
            return fused(mesh, grad_iterate, scale)
        return general(grad_iterate, scale)

    def whole(grad_iterate):
        scale = math.sqrt(grad_iterate.shape[1])
        return jax.shard_map(
            functools.partial(local, scale),
            mesh=mesh,
            in_specs=(P("tp", "fsdp"),),
            out_specs=P("tp", "fsdp"),
            check_vma=False,
        )(grad_iterate)

    return whole
```

```python
import functools
import math

import jax
import jax.numpy as jnp
from jax import lax
from jax.experimental import pallas as pl
from jax.experimental.pallas import tpu as pltpu
from jax.sharding import PartitionSpec as P

quintic_one = 3.4445
quintic_three = -4.775
quintic_five = 2.0315

MESH = pl.DeviceIdType.MESH


def rows_by_rows(a, b):
    return lax.dot_general(a, b, (((1,), (1,)), ((), ())), preferred_element_type=jnp.float32)


def columns_by_rows(a, b):
    return lax.dot_general(a, b, (((0,), (0,)), ((), ())), preferred_element_type=jnp.float32)


def matmul(a, b):
    return jnp.dot(a, b, preferred_element_type=jnp.float32)


def general(grad_iterate, scale):
    columns = lax.all_gather(grad_iterate, "tp", axis=0, tiled=True)
    shares = lax.psum_scatter(
        rows_by_rows(columns, grad_iterate), "fsdp", scatter_dimension=0, tiled=True
    )
    gram_cols = lax.all_gather(shares.astype(jnp.bfloat16), "fsdp", axis=0, tiled=True)
    applied = lax.dot_general(
        gram_cols, columns, (((0,), (0,)), ((), ())), preferred_element_type=jnp.float32
    )
    twice_applied = matmul(
        gram_cols.T, lax.all_gather(applied.astype(jnp.bfloat16), "tp", axis=0, tiled=True)
    )
    mixed = (
        quintic_one * grad_iterate.astype(jnp.float32)
        + quintic_three * applied
        + quintic_five * twice_applied
    )
    return mixed * scale


def fused_kernel(
    nz, tile, scale,
    x_hbm, o_hbm,
    xg, xp, gram, acc, dxs, dxr, dzs, dzr, cxs, cxr, czs, czr,
    local_sem, ys, yr, cs, cr, dx_s, dx_r, dz_s, dz_r, cx_s, cx_r, cz_s, cz_r,
    daz_s, daz_r, dax_s, dax_r, dac_s, dac_r, dly_s, dly_r, dlc_s, dlc_r,
    cay_s, cay_r, caz_s, caz_r, cax_s, cax_r, cac_s, cac_r, out_sem,
):
    f = lax.axis_index("fsdp")
    y = lax.axis_index("tp")
    c = lax.rem(f, 2)
    xx = lax.rem(f // 2, 2)
    z = f // 4

    rows = xg.shape[1]
    half = rows // 2
    quarter = half // 2
    dpiece = half // nz
    cpiece = quarter // nz

    def device(z_, x_, c_, y_):
        return (z_ * 4 + x_ * 2 + c_, y_)

    to_y = device(z, xx, c, 1 - y)
    to_x = device(z, 1 - xx, c, y)
    to_c = device(z, xx, 1 - c, y)
    to_z = [device(lax.rem(z + k, nz), xx, c, y) for k in range(1, nz)]

    def remote(src, dst, ssem, rsem, target):
        return pltpu.make_async_remote_copy(
            src_ref=src, dst_ref=dst, send_sem=ssem, recv_sem=rsem,
            device_id=target, device_id_type=MESH,
        )

    load = pltpu.make_async_copy(x_hbm, xg.at[y], local_sem)
    load.start()
    barrier = pltpu.get_barrier_semaphore()
    peers = [to_y, to_x, to_c] + to_z
    for peer in peers:
        pl.semaphore_signal(barrier, inc=1, device_id=peer, device_id_type=MESH)
    pl.semaphore_wait(barrier, len(peers))
    load.wait()

    sends = []

    def begin(copy):
        copy.start()
        sends.append(copy)
        return copy

    def move(block, ssem, rsem, target):
        return begin(remote(block, block, ssem, rsem, target))

    def at(i, n):
        return pl.ds(pl.multiple_of(i, n if n < 128 else 16), n)

    def back_from(k):
        return lax.rem(z - k + nz, nz)

    share = begin(remote(xg.at[y], xp.at[y], cs.at[0], cr.at[0], to_c))

    def x_block(s):
        h = (1 - y) if s < 2 else y
        return xg.at[y, at(h * half + (s % 2) * quarter, quarter)]

    over = [move(x_block(s), ys.at[s], yr.at[s], to_y) for s in range(4)]
    share.wait_recv()

    cols = pl.ds(pl.multiple_of(c * half, 128), half)
    rhs = at(c * half, half)

    def gram_part(left, lrow, n, right):
        l = at(lrow, n)
        return rows_by_rows(xg[left, l, :], xg[right, rhs, :]) + rows_by_rows(
            xp[left, l, :], xp[right, rhs, :]
        )

    def order(p):
        return lax.rem(z + 1 + p, nz)

    def d_copy(p):
        t = order(p)
        return remote(dxs.at[t], dxr.at[t], dx_s.at[p], dx_r.at[p], to_x)

    def d_send(p, _):
        t = order(p)
        dxs[t] = gram_part(y, (1 - xx) * half + t * dpiece, dpiece, y).astype(jnp.bfloat16)
        d_copy(p).start()
        return 0

    lax.fori_loop(0, nz, d_send, 0)

    def d_own(p, _):
        t = order(p)
        acc[y, at(t * dpiece, dpiece), 0:half] = gram_part(
            y, xx * half + t * dpiece, dpiece, y
        )
        return 0

    lax.fori_loop(0, nz, d_own, 0)

    dz = []
    for p in range(nz):
        t = order(p)
        d_copy(p).wait()
        place = at(t * dpiece, dpiece)
        total = acc[y, place, 0:half] + dxr[t].astype(jnp.float32)
        if p < nz - 1:
            dzs[p] = total.astype(jnp.bfloat16)
            dz.append(begin(remote(dzs.at[p], dzr.at[p], dz_s.at[p], dz_r.at[p], to_z[p])))
        else:
            acc[y, place, 0:half] = total

    for s in range(2):
        over[s].wait_recv()
    fwd = (1 - y) * (1 - c) + y
    block = at(fwd * half, half)
    cfwd = remote(xg.at[1 - y, block], xp.at[1 - y, block], cs.at[1], cr.at[1], to_c)
    sends.append(cfwd)
    late_send = jnp.logical_and(y == 0, c == 0)
    late_c = jnp.logical_and(y == 0, c == 1)

    @pl.when(jnp.logical_not(late_send))
    def _():
        cfwd.start()

    def c_copy(t):
        return remote(cxs.at[t], cxr.at[t], cx_s.at[t], cx_r.at[t], to_x)

    def cz_copy(p):
        return remote(czs.at[p], czr.at[p], cz_s.at[p], cz_r.at[p], to_z[p])

    def c_compute():
        cfwd.wait_recv()
        part = gram_part(0, y * half + (1 - xx) * quarter, quarter, 1)
        for t in range(nz):
            cxs[t] = part[t * cpiece:(t + 1) * cpiece].astype(jnp.bfloat16)
        for t in range(nz):
            c_copy(t).start()
        acc[1 - y, 0:quarter, 0:half] = gram_part(0, y * half + xx * quarter, quarter, 1)

    def c_exchange():
        for t in range(nz):
            c_copy(t).wait()
        for p in range(nz - 1):
            t = order(p)
            czs[p] = (
                acc[1 - y, at(t * cpiece, cpiece), 0:half] + cxr[t].astype(jnp.float32)
            ).astype(jnp.bfloat16)
            cz_copy(p).start()

    def c_slab(who, x_, z_):
        return (1, at(who * half + x_ * quarter + z_ * cpiece, cpiece), cols)

    cmine = gram.at[c_slab(y, xx, z)]
    cay = remote(cmine, cmine, cay_s, cay_r, to_y)

    def c_finish():
        total = acc[1 - y, at(z * cpiece, cpiece), 0:half] + cxr[z].astype(jnp.float32)
        for p in range(nz - 1):
            cz_copy(p).wait()
            total = total + czr[p].astype(jnp.float32)
        gram[c_slab(y, xx, z)] = total.astype(jnp.bfloat16)
        cay.start()

    @pl.when(jnp.logical_not(late_c))
    def _():
        c_compute()

    def d_slab(who, x_, z_):
        return (2 * who, at(x_ * half + z_ * dpiece, dpiece), cols)

    total = acc[y, at(z * dpiece, dpiece), 0:half]
    for p in range(nz - 1):
        dz[p].wait_recv()
        total = total + dzr[p].astype(jnp.float32)
    gram[d_slab(y, xx, z)] = total.astype(jnp.bfloat16)

    daz, dax, dac, dly, dlc = [], [], [], [], []

    def pass_own(k):
        here = gram.at[d_slab(y, xx, back_from(k))]
        dax.append(move(here, dax_s.at[k], dax_r.at[k], to_x))
        dac.append(move(here, dac_s.at[k], dac_r.at[k], to_c))

    def pass_late(k):
        here = gram.at[d_slab(y, xx if k < nz else 1 - xx, back_from(k % nz))]
        dly.append(move(here, dly_s.at[k], dly_r.at[k], to_y))

    dmine = gram.at[d_slab(y, xx, z)]

    def spread_own(k):
        daz.append(move(dmine, daz_s.at[k], daz_r.at[k], to_z[k]))

    pass_own(0)
    spread_own(0)

    @pl.when(jnp.logical_not(late_c))
    def _():
        c_exchange()

    for k in range(1, nz - 1):
        spread_own(k)
    daz[0].wait_recv()
    pass_own(1)

    @pl.when(jnp.logical_not(late_c))
    def _():
        c_finish()

    pass_late(0)
    pass_late(1)

    def c_move(who, k, target, ssem, rsem):
        here = gram.at[c_slab(who, xx, back_from(k))]
        return remote(here, here, ssem, rsem, target)

    def c_over_z(who, k):
        j = who * (nz - 1) + k
        return c_move(who, 0, to_z[k], caz_s.at[j], caz_r.at[j])

    def c_over_x(who, k):
        j = who * nz + k
        return c_move(who, k, to_x, cax_s.at[j], cax_r.at[j])

    def c_over_c(who, k):
        j = who * nz + k
        return c_move(who, k, to_c, cac_s.at[j], cac_r.at[j])

    def c_spread(who):
        @pl.when(y == 1 - who)
        def _():
            cay.wait_recv()

        for k in range(nz - 1):
            c_over_z(who, k).start()
        c_over_x(who, 0).start()
        c_over_c(who, 0).start()

    for s in range(2, 4):
        over[s].wait_recv()

    @pl.when(late_send)
    def _():
        cfwd.start()

    @pl.when(late_c)
    def _():
        c_compute()

    c_spread(1)

    @pl.when(c == 0)
    def _():
        c_spread(0)

    for k in range(2, nz):
        daz[k - 1].wait_recv()
        pass_own(k)
        pass_late(k)

    @pl.when(late_c)
    def _():
        c_exchange()

    def d_from_x(k):
        dax[k].wait_recv()
        here = gram.at[d_slab(y, 1 - xx, back_from(k))]
        dac.append(move(here, dac_s.at[nz + k], dac_r.at[nz + k], to_c))

    for k in range(nz - 1):
        d_from_x(k)
    pass_late(nz)

    @pl.when(late_c)
    def _():
        c_finish()

    for k in range(1, nz - 1):
        pass_late(nz + k)

    @pl.when(c == 1)
    def _():
        c_spread(0)

    d_from_x(nz - 1)
    pass_late(2 * nz - 1)
    for copy in dac:
        copy.wait_recv()

    def tile_of(i):
        return at(i * tile, tile)

    tiles = rows // tile

    def clear(i, _):
        acc[1 - y, tile_of(i), :] = jnp.zeros((tile, acc.shape[2]), jnp.float32)
        return 0

    lax.fori_loop(0, tiles, clear, 0)

    def diagonal(first, count):
        def body(i, _):
            m = tile_of(i)
            acc[y, m, :] = matmul(gram[2 * y, m, :], xg[y])
            return 0

        lax.fori_loop(first, first + count, body, 0)

    def share_out(events):
        done = 0
        for n, event in enumerate(events):
            upto = tiles * (n + 1) // len(events)
            if upto > done:
                diagonal(done, upto - done)
            done = upto
            event()

    def c_pass(who, k):
        def event():
            c_over_z(who, k - 1).wait_recv()
            c_over_x(who, k).start()
            c_over_c(who, k).start()

        return event

    def d_late(k):
        dly[k].wait_recv()
        here = gram.at[d_slab(1 - y, xx if k < nz else 1 - xx, back_from(k % nz))]
        dlc.append(move(here, dlc_s.at[k], dlc_r.at[k], to_c))

    def d_other(k):
        dlc[k].wait_recv()
        r = at((xx if k < nz else 1 - xx) * half + back_from(k % nz) * dpiece, dpiece)
        total = acc[1 - y, r, :] + matmul(gram[2 * (1 - y), r, :], xg[1 - y])
        acc[1 - y, r, :] = total
        xp[1 - y, r, :] = total.astype(jnp.bfloat16)

    def c_from_x(who, k):
        def event():
            c_over_x(who, k).wait_recv()
            j = (2 + who) * nz + k
            here = gram.at[c_slab(who, 1 - xx, back_from(k))]
            far[who].append(move(here, cac_s.at[j], cac_r.at[j], to_c))

        return event

    def cross(x_, who, last):
        m = at(who * half + x_ * quarter, quarter)
        total = acc[0, m, :] + matmul(gram[1, m, :], xg[1])
        acc[0, m, :] = total
        xp[0, m, :] = total.astype(jnp.bfloat16)

        def body(i, _):
            n = tile_of(i)
            ncol = pl.ds(pl.multiple_of(i * tile, 128), tile)
            total = acc[1, n, :] + columns_by_rows(gram[1, m, ncol], xg[0, m, :])
            acc[1, n, :] = total
            if last:
                xp[1, n, :] = total.astype(jnp.bfloat16)
            return 0

        lax.fori_loop(0, tiles, body, 0)

    def cross_own(who):
        for k in range(nz):
            c_over_c(who, k).wait_recv()
        cross(xx, who, False)

    def cross_far(who, last):
        for copy in far[who]:
            copy.wait_recv()
        cross(1 - xx, who, last)

    far = [[], []]
    share_out([c_pass(1, k) for k in range(1, nz)])
    for k in range(1, nz):
        c_pass(0, k)()
    for k in range(nz):
        c_from_x(1, k)()
    for k in range(nz):
        d_late(k)
    cross_own(1)
    cross_far(1, False)
    for k in range(nz):
        c_from_x(0, k)()
    for k in range(nz):
        d_other(k)
    for k in range(nz, 2 * nz - 2):
        d_late(k)
    cross_own(0)
    cross_far(0, True)
    for k in range(nz, 2 * nz - 2):
        d_other(k)
    def near(i, _):
        m = tile_of(i)
        acc[y, m, :] = (
            quintic_one * xg[y, m, :].astype(jnp.float32)
            + quintic_three * acc[y, m, :]
            + quintic_five * matmul(gram[2 * y, m, :], xp[y])
        )
        return 0

    lax.fori_loop(0, tiles, near, 0)
    for k in range(2 * nz - 2, 2 * nz):
        d_late(k)
        d_other(k)

    def back(i):
        m = tile_of(i)
        return pltpu.make_async_copy(acc.at[y, m], o_hbm.at[m], out_sem.at[i])

    @pl.when(y == 0)
    def _():
        def body(i, _):
            m = tile_of(i)
            acc[0, m, :] = (acc[0, m, :] + quintic_five * matmul(gram[1, m, :], xp[1])) * scale
            back(i).start()
            return 0

        lax.fori_loop(0, tiles, body, 0)

    @pl.when(y == 1)
    def _():
        def body(i, _):
            m = tile_of(i)
            ncol = pl.ds(pl.multiple_of(i * tile, 128), tile)
            acc[1, m, :] = (
                acc[1, m, :] + quintic_five * columns_by_rows(gram[1, :, ncol], xp[0])
            ) * scale
            back(i).start()
            return 0

        lax.fori_loop(0, tiles, body, 0)

    for who in range(2):
        for k in range(nz - 1):
            sends.append(c_over_z(who, k))
        for k in range(nz):
            sends += [c_over_x(who, k), c_over_c(who, k)]
    for copy in sends + [cay]:
        copy.wait_send()

    def drain(i, _):
        back(i).wait()
        return 0

    lax.fori_loop(0, rows // tile, drain, 0)


def fused(mesh, grad_iterate, scale):
    rows, width = grad_iterate.shape
    nz = mesh.shape["fsdp"] // 4
    half, quarter = rows // 2, rows // 4
    dpiece, cpiece = half // nz, quarter // nz
    tile = next(t for t in (256, 128) if rows % t == 0)
    bf16, f32 = jnp.bfloat16, jnp.float32
    dma = pltpu.SemaphoreType.DMA
    scratch = [
        pltpu.VMEM((2, rows, width), bf16),
        pltpu.VMEM((2, rows, width), bf16),
        pltpu.VMEM((3, rows, rows), bf16),
        pltpu.VMEM((2, rows, width), f32),
        pltpu.VMEM((nz, dpiece, half), bf16),
        pltpu.VMEM((nz, dpiece, half), bf16),
        pltpu.VMEM((nz - 1, dpiece, half), bf16),
        pltpu.VMEM((nz - 1, dpiece, half), bf16),
        pltpu.VMEM((nz, cpiece, half), bf16),
        pltpu.VMEM((nz, cpiece, half), bf16),
        pltpu.VMEM((nz - 1, cpiece, half), bf16),
        pltpu.VMEM((nz - 1, cpiece, half), bf16),
        dma,
    ]
    counts = dict(
        y=4, c=2, dx=nz, dz=nz - 1, cx=nz, cz=nz - 1, daz=nz - 1,
        dax=nz, dac=2 * nz, dly=2 * nz, dlc=2 * nz,
        cay=None, caz=2 * (nz - 1), cax=2 * nz, cac=4 * nz,
    )
    for count in counts.values():
        scratch += [dma if count is None else dma((count,))] * 2
    scratch.append(dma((rows // tile,)))
    flops = 2 * rows * rows * width * 7
    return pl.pallas_call(
        functools.partial(fused_kernel, nz, tile, scale),
        out_shape=jax.ShapeDtypeStruct((rows, width), f32),
        in_specs=[pl.BlockSpec(memory_space=pl.ANY)],
        out_specs=pl.BlockSpec(memory_space=pl.ANY),
        scratch_shapes=scratch,
        compiler_params=pltpu.CompilerParams(
            collective_id=0, has_side_effects=True, vmem_limit_bytes=67043328
        ),
        cost_estimate=pl.CostEstimate(
            flops=flops, bytes_accessed=6 * rows * width, transcendentals=0
        ),
    )(grad_iterate)


def fits(mesh, shape):
    rows, width = shape
    devices = mesh.shape["fsdp"]
    if mesh.shape["tp"] != 2 or devices % 4 or devices < 8:
        return False
    nz = devices // 4
    if rows % 256 or rows // 2 > width or width % 128 or (rows // 4) % (16 * nz):
        return False
    return 16 * rows * width + 8 * rows * rows < 60 * 2**20


def solution(mesh):
    def local(scale, grad_iterate):
        if fits(mesh, grad_iterate.shape):
            return fused(mesh, grad_iterate, scale)
        return general(grad_iterate, scale)

    def whole(grad_iterate):
        scale = math.sqrt(grad_iterate.shape[1])
        return jax.shard_map(
            functools.partial(local, scale),
            mesh=mesh,
            in_specs=(P("tp", "fsdp"),),
            out_specs=P("tp", "fsdp"),
            check_vma=False,
        )(grad_iterate)

    return whole
```
